32 devices in a mesh: inst: 4 (over x, core), gx: 2 (over y), gy: 4 (over z).
Axes of the slice: x: 2, y: 2, z: 4, core: 2. Of those that a mesh axis runs over, the one named last changes fastest.
Arguments:
- state: float32 [8, 5, 16, 32, 128], P('inst', None, 'gx', 'gy'), may hold values from -6 to 6
- source: float32 [8, 5, 16, 32, 128], P('inst', None, 'gx', 'gy'), may hold values from -60 to 60
- jacobian: float32 [8, 5, 5, 16, 32, 128], P('inst', None, None, 'gx', 'gy'), may hold values from -1.5 to 16, as said below
- couplings: float32 [6, 5, 5], replicated, may hold values from -0.625 to 0.625
- omega: float32 [1], replicated, may hold values from 0.2 to 0.6
Outputs:
- state_next: float32 [8, 5, 16, 32, 128], P('inst', None, 'gx', 'gy')
- last_residual: float32 [8, 5, 16, 32, 128], P('inst', None, 'gx', 'gy')
The draws below stay inside these ranges and needn't reach their ends.
Inputs may be any that keep to these rules, and one draw needn't show every extreme that they name: In every block jacobian[n, :, :, cell] each diagonal entry lies in 8 to 16 and exceeds the sum of magnitudes of the other entries of its row by 2 or more.
All inputs are finite; a program needn't handle non-finite values.
Results may differ from the reference program's by a relative error of at most 0.0003.
Values sent between devices are 32-bit elements; how exact they have to be, the bound alone decides.
No kernel may reach another device: no remote copies, remote signals or barrier semaphores. Data moves between devices by JAX's collectives and lax.ppermute only.
A program may use at most 64 MiB of HBM per device.

```python
import math
import jax
import jax.numpy as jnp
from jax import lax

NVAR = 5
NT = 8
ITERS = 3
NX = 16
NY = 32
NZ = 128


def draw_jacobian(key, part):
    first_key, second_key = jax.random.split(jax.random.fold_in(key, 17))
    shape = (NT, NVAR, NVAR, NX, NY, NZ)
    diagonal = jax.random.uniform(first_key, (NT, NVAR, NX, NY, NZ), jnp.float32, 8.0, 16.0)
    others = jnp.clip(0.6 * jax.random.normal(second_key, shape, jnp.float32), -1.5, 1.5)
    identity = jnp.eye(NVAR, dtype=jnp.float32)[None, :, :, None, None, None]
    return others * (1.0 - identity) + identity * diagonal[:, :, None]


def shard_levels(stream_key, shape, shards, least, largest):
    level, own = 1.0, jax.random.fold_in(stream_key, 6)
    for axis_at, blocks in shards:
        heights = jnp.exp(jax.random.uniform(jax.random.fold_in(own, axis_at), (blocks,), jnp.float32, least / len(shards), largest / len(shards)))
        level = level * jnp.repeat(heights, shape[axis_at] // blocks).reshape([-1 if axis == axis_at else 1 for axis in range(len(shape))])
    return level


def bell_draw(key, shape, scale, most, cuts=(), held_as=jnp.bfloat16):
    drawn = scale * jax.random.normal(key, shape, jnp.float32)
    if cuts:
        drawn = drawn * shard_levels(key, shape, cuts, -0.22, 0.18)
    return jnp.clip(drawn, -most, most).astype(held_as)


def setup_inputs(seed: int = 0) -> dict:
    streams_of = jax.random.split(jax.random.key(seed), 6)
    return {
        "state": bell_draw(streams_of[0], (NT, NVAR, NX, NY, NZ), 1.0, 6.0, ((0, 4), (2, 2), (3, 4)), jnp.float32),
        "source": bell_draw(streams_of[1], (NT, NVAR, NX, NY, NZ), 10.0, 60.0, ((0, 4), (2, 2), (3, 4)), jnp.float32),
        "jacobian": draw_jacobian(jax.random.fold_in(streams_of[5], 71), 0),
        "couplings": bell_draw(streams_of[3], (6, NVAR, NVAR), 100 ** -0.5, 0.625, (), jnp.float32),
        "omega": jnp.clip(jnp.exp(jax.random.uniform(streams_of[4], (1,), jnp.float32, math.log(0.2), math.log(0.6))), 0.2, 0.6),
    }


def spectral_table(row_index, column_index, total):
    offset = (row_index[:, None] - column_index[None, :]).astype(jnp.int32)
    parity = 1.0 - 2.0 * jnp.mod(offset, 2).astype(jnp.float32)
    angle = jnp.pi * offset.astype(jnp.float32) / total
    onsite = offset == 0
    sine = jnp.where(onsite, jnp.ones_like(angle), jnp.sin(angle))
    return jnp.where(onsite, jnp.zeros_like(angle), 0.5 * parity * jnp.cos(angle) / sine)


def pad_field(field):
    wrapped = jnp.concatenate([field[:, :, -1:], field, field[:, :, :1]], axis=2)
    return jnp.pad(wrapped, ((0, 0), (1, 1), (0, 0), (1, 1)))


def neighbours(padded, couplings):
    shifted = [padded[:, :-2, 1:-1, 1:-1], padded[:, 2:, 1:-1, 1:-1],
               padded[:, 1:-1, :-2, 1:-1], padded[:, 1:-1, 2:, 1:-1],
               padded[:, 1:-1, 1:-1, :-2], padded[:, 1:-1, 1:-1, 2:]]
    result = jnp.zeros(shifted[0].shape, jnp.float32)
    for direction in range(6):
        result = result + jnp.einsum("vw,wxyz->vxyz", couplings[direction], shifted[direction],
                                     precision=lax.Precision.HIGHEST)
    return result


def solve_blocks(blocks, right):
    size = blocks.shape[0]
    matrix = [[blocks[row, column] for column in range(size)] for row in range(size)]
    vector = [right[row] for row in range(size)]
    for pivot in range(size):
        for target in range(pivot + 1, size):
            factor = matrix[target][pivot] / matrix[pivot][pivot]
            for column in range(pivot + 1, size):
                matrix[target][column] = matrix[target][column] - factor * matrix[pivot][column]
            vector[target] = vector[target] - factor * vector[pivot]
    result = [None] * size
    for pivot in reversed(range(size)):
        total = vector[pivot]
        for column in range(pivot + 1, size):
            total = total - matrix[pivot][column] * result[column]
        result[pivot] = total / matrix[pivot][pivot]
    return jnp.stack(result, axis=0)


def reference(state, source, jacobian, couplings, omega):
    total = state.shape[0]
    positions = jnp.arange(total, dtype=jnp.int32)
    table = spectral_table(positions, positions, total)
    current = state
    residual = state
    for repeat in range(ITERS):
        spectral = omega[0] * jnp.einsum("nm,mvxyz->nvxyz", table, current,
                                         precision=lax.Precision.HIGHEST)

        def one_instance(pieces):
            field, blocks, right_side, spec_part = pieces
            beside = neighbours(pad_field(field), couplings)
            diagonal_part = jnp.einsum("vwxyz,wxyz->vxyz", blocks, field,
                                       precision=lax.Precision.HIGHEST)
            resid = right_side - diagonal_part - beside - spec_part
            return field + solve_blocks(blocks, resid), resid

        current, residual = lax.map(one_instance, (current, jacobian, source, spectral))
    return current, residual
```

```python
import functools
import math

import jax
import jax.numpy as jnp
import numpy as np
from jax import lax
from jax.experimental import pallas as pl
from jax.experimental.pallas import tpu as pltpu
from jax.sharding import PartitionSpec as P

ITERS = 3
GROUP = 4
LIMIT = 16 * 2**20

VMEM = pl.BlockSpec(memory_space=pltpu.VMEM)
SMEM = pl.BlockSpec(memory_space=pltpu.SMEM)


def table_of(total):
    table = np.zeros((total, total))
    for n in range(total):
        for m in range(total):
            if n != m:
                angle = math.pi * (n - m) / total
                table[n, m] = 0.5 * (-1.0) ** (n - m) * math.cos(angle) / math.sin(angle)
    return table.astype(np.float32)


def weights(ranks, local, slot, omega):
    table = table_of(ranks * local)
    rank = lax.axis_index("inst")
    result = []
    for i in range(local):
        row = []
        for j in range(local):
            if slot == 0 and i == j:
                row.append(None)
                continue
            value = jnp.float32(table[i, slot * local + j])
            for r in range(1, ranks):
                entry = jnp.float32(table[r * local + i, (r ^ slot) * local + j])
                value = jnp.where(rank == r, entry, value)
            row.append(omega * value)
        result.append(row)
    return result


def lu_body(jac, lu):
    local, size, _, extent_x = jac.shape[:4]
    for n in range(local):
        for x in range(extent_x):
            m = [[jac[n, i, j, x] for j in range(size)] for i in range(size)]
            for p in range(size):
                m[p][p] = 1.0 / m[p][p]
                for t in range(p + 1, size):
                    m[t][p] = m[t][p] * m[p][p]
                    for c in range(p + 1, size):
                        m[t][c] = m[t][c] - m[t][p] * m[p][c]
            for i in range(size):
                for j in range(size):
                    lu[n, i, j, x] = m[i][j]


def store_faces(field, n, v, x, extent_x, count, faces):
    first, last = faces[-2:]
    first[n, v, x] = field[0]
    last[n, v, x] = field[-1]
    if count == 2:
        own = lax.axis_index("gx")
        if x == extent_x - 1:

            @pl.when(own == 0)
            def _():
                faces[0][n, v] = field

        if x == 0:

            @pl.when(own == 1)
            def _():
                faces[0][n, v] = field
    else:
        if x == 0:
            faces[0][n, v] = field
        if x == extent_x - 1:
            faces[1][n, v] = field


def faces_body(count, u, *faces):
    local, size, extent_x = u.shape[:3]
    for n in range(local):
        for v in range(size):
            for x in range(extent_x):
                store_faces(u[n, v, x], n, v, x, extent_x, count, faces)


def near_body(count, ranks, final, omega, coup, u, *refs):
    near, refs = (refs[0], refs[1:]) if ranks > 1 else (None, refs)
    if count == 2:
        gx, refs = refs[:1], refs[1:]
    else:
        gx, refs = refs[:2], refs[2:]
    low_y, high_y, source, refs = refs[0], refs[1], refs[2], refs[3:]
    if final:
        jac, out, product = refs
    else:
        (out,) = refs
    local, size, extent_x, extent_y, extent_z = u.shape
    own = lax.axis_index("gx")
    row_at = lax.broadcasted_iota(jnp.int32, (extent_y, extent_z), 0)
    lane_at = lax.broadcasted_iota(jnp.int32, (extent_y, extent_z), 1)
    table = [weights(ranks, local, 0, omega[0])]
    fields = [u]
    if ranks > 1:
        table.append(weights(ranks, local, 1, omega[0]))
        fields.append(near)
    group = math.gcd(GROUP, extent_x)

    def beyond(n, w, side):
        if count == 2:
            return jnp.where(own == 1 - side, gx[0][n, w], 0.0)
        return gx[side][n, w]

    for n in range(local):
        for start in range(0, extent_x, group):
            rows = range(start, start + group)
            acc = [[source[n, v, x] for x in rows] for v in range(size)]
            for w in range(size):
                cells = [u[n, w, x] for x in rows]
                below = [u[n, w, start - 1] if start else beyond(n, w, 0)] + cells[:-1]
                above = cells[1:] + [
                    u[n, w, start + group] if start + group < extent_x else beyond(n, w, 1)
                ]
                around = [
                    below,
                    above,
                    [
                        jnp.where(row_at == 0, low_y[n, w, x][None], pltpu.roll(c, 1, 0))
                        for x, c in zip(rows, cells)
                    ],
                    [
                        jnp.where(
                            row_at == extent_y - 1,
                            high_y[n, w, x][None],
                            pltpu.roll(c, extent_y - 1, 0),
                        )
                        for x, c in zip(rows, cells)
                    ],
                    [jnp.where(lane_at == 0, 0.0, pltpu.roll(c, 1, 1)) for c in cells],
                    [
                        jnp.where(lane_at == extent_z - 1, 0.0, pltpu.roll(c, extent_z - 1, 1))
                        for c in cells
                    ],
                ]
                for d in range(6):
                    for v in range(size):
                        factor = coup[d, v, w]
                        for k in range(group):
                            acc[v][k] = acc[v][k] - factor * around[d][k]
            for field, part in zip(fields, table):
                for j in range(local):
                    factor = part[n][j]
                    if factor is None:
                        continue
                    for v in range(size):
                        for k, x in enumerate(rows):
                            acc[v][k] = acc[v][k] - factor * field[j, v, x]
            for v in range(size):
                for k, x in enumerate(rows):
                    out[n, v, x] = acc[v][k]
            if final:
                for k, x in enumerate(rows):
                    for v in range(size):
                        total = jac[n, v, 0, x] * u[n, 0, x]
                        for w in range(1, size):
                            total = total + jac[n, v, w, x] * u[n, w, x]
                        product[n, v, x] = total


def far_body(count, ranks, final, omega, part, lu, *refs):
    far, refs = refs[: max(ranks - 2, 0)], refs[max(ranks - 2, 0) :]
    if final:
        product, out, resid = refs
    else:
        out, faces = refs[0], refs[1:]
    local, size, extent_x = part.shape[:3]
    table = [weights(ranks, local, slot, omega[0]) for slot in range(2, ranks)]
    group = math.gcd(GROUP, extent_x)
    for n in range(local):
        for start in range(0, extent_x, group):
            rows = range(start, start + group)
            right = [[part[n, v, x] for x in rows] for v in range(size)]
            for field, entry in zip(far, table):
                for j in range(local):
                    for v in range(size):
                        for k, x in enumerate(rows):
                            right[v][k] = right[v][k] - entry[n][j] * field[j, v, x]
            if final:
                for v in range(size):
                    for k, x in enumerate(rows):
                        resid[n, v, x] = right[v][k] - product[n, v, x]
            for k, x in enumerate(rows):
                vector = [right[v][k] for v in range(size)]
                for p in range(size):
                    for t in range(p + 1, size):
                        vector[t] = vector[t] - lu[n, t, p, x] * vector[p]
                for p in reversed(range(size)):
                    for c in range(p + 1, size):
                        vector[p] = vector[p] - lu[n, p, c, x] * vector[c]
                    vector[p] = vector[p] * lu[n, p, p, x]
                for v in range(size):
                    out[n, v, x] = vector[v]
                    if not final:
                        store_faces(vector[v], n, v, x, extent_x, count, faces)


def call(body, name, smem, outs, *args):
    return pl.pallas_call(
        body,
        out_shape=outs,
        in_specs=[SMEM] * smem + [VMEM] * (len(args) - smem),
        out_specs=[VMEM] * len(outs),
        compiler_params=pltpu.CompilerParams(vmem_limit_bytes=LIMIT),
        name=name,
    )(*args)


def shards(state, source, jacobian, couplings, omega):
    ranks = lax.axis_size("inst")
    count_x = lax.axis_size("gx")
    count_y = lax.axis_size("gy")
    local, size, extent_x, extent_y, extent_z = state.shape
    assert ranks & (ranks - 1) == 0

    def shape(*dims):
        return jax.ShapeDtypeStruct(dims, jnp.float32)

    face_x = shape(local, size, extent_y, extent_z)
    face_y = shape(local, size, extent_x, extent_z)
    face_shapes = [face_x] * (1 if count_x == 2 else 2) + [face_y] * 2
    full = shape(*state.shape)

    def swap(field, bit):
        return lax.ppermute(field, "inst", [(r, r ^ bit) for r in range(ranks)])

    def exchange(faces):
        ring = [(r, (r + 1) % count_y) for r in range(count_y)]
        back = [(b, a) for a, b in ring]
        first, last = faces[-2:]
        low_y = lax.ppermute(last, "gy", ring)
        high_y = lax.ppermute(first, "gy", back)
        line = [(r, r + 1) for r in range(count_x - 1)]
        if count_x == 2:
            gx = [lax.ppermute(faces[0], "gx", [(0, 1), (1, 0)])]
        else:
            gx = [
                lax.ppermute(faces[1], "gx", line),
                lax.ppermute(faces[0], "gx", [(b, a) for a, b in line]),
            ]
        return gx + [low_y, high_y]

    current = state
    faces = call(functools.partial(faces_body, count_x), "faces", 0, face_shapes, state)
    (lu,) = call(lu_body, "factor", 0, [shape(*jacobian.shape)], jacobian)
    for repeat in range(ITERS):
        final = repeat == ITERS - 1
        slots = {0: current}
        bit = ranks // 2
        while bit > 1:
            slots.update({slot | bit: swap(field, bit) for slot, field in slots.items()})
            bit //= 2
        if ranks > 1:
            slots[1] = swap(current, 1)
        around = exchange(faces)
        near = [slots[1]] if ranks > 1 else []
        parts = call(
            functools.partial(near_body, count_x, ranks, final),
            "near",
            2,
            [full] * (2 if final else 1),
            omega,
            couplings,
            current,
            *near,
            *around,
            source,
            *([jacobian] if final else []),
        )
        others = [slots[slot] for slot in range(2, ranks, 2)]
        lu, parts, others = lax.optimization_barrier((lu, parts, others))
        for slot, field in zip(range(2, ranks, 2), others):
            slots[slot] = field
            slots[slot | 1] = swap(field, 1)
        results = call(
            functools.partial(far_body, count_x, ranks, final),
            "far",
            1,
            [full, full] if final else [full] + face_shapes,
            omega,
            parts[0],
            lu,
            *[slots[slot] for slot in range(2, ranks)],
            *parts[1:],
        )
        current, faces = results[0], results[1:]
    return (current, faces[0])


def solution(mesh):
    return jax.shard_map(
        shards,
        mesh=mesh,
        in_specs=(
            P("inst", None, "gx", "gy", None),
            P("inst", None, "gx", "gy", None),
            P("inst", None, None, "gx", "gy", None),
            P(),
            P(),
        ),
        out_specs=(P("inst", None, "gx", "gy", None), P("inst", None, "gx", "gy", None)),
        check_vma=False,
    )
```

```python
import functools
import math

import jax
import jax.numpy as jnp
import numpy as np
from jax import lax
from jax.experimental import pallas as pl
from jax.experimental.pallas import tpu as pltpu
from jax.sharding import PartitionSpec as P


ITERS = 3
GROUP = 4
LIMIT = 16 * 2**20

VMEM = pl.BlockSpec(memory_space=pltpu.VMEM)
SMEM = pl.BlockSpec(memory_space=pltpu.SMEM)


def table_of(total):
    table = np.zeros((total, total))
    for n in range(total):
        for m in range(total):
            if n != m:
                angle = math.pi * (n - m) / total
                table[n, m] = 0.5 * (-1.0) ** (n - m) * math.cos(angle) / math.sin(angle)
    return table.astype(np.float32)


def weights(ranks, local, slot, omega):
    table = table_of(ranks * local)
    rank = lax.axis_index("inst")
    result = []
    for i in range(local):
        row = []
        for j in range(local):
            if slot == 0 and i == j:
                row.append(None)
                continue
            value = jnp.float32(table[i, slot * local + j])
            for r in range(1, ranks):
                entry = jnp.float32(table[r * local + i, (r ^ slot) * local + j])
                value = jnp.where(rank == r, entry, value)
            row.append(omega * value)
        result.append(row)
    return result


def lu_body(jac, lu):
    local, size, _, extent_x = jac.shape[:4]
    for n in range(local):
        for x in range(extent_x):
            m = [[jac[n, i, j, x] for j in range(size)] for i in range(size)]
            for p in range(size):
                m[p][p] = 1.0 / m[p][p]
                for t in range(p + 1, size):
                    m[t][p] = m[t][p] * m[p][p]
                    for c in range(p + 1, size):
                        m[t][c] = m[t][c] - m[t][p] * m[p][c]
            for i in range(size):
                for j in range(size):
                    lu[n, i, j, x] = m[i][j]


def store_faces(field, n, v, x, extent_x, count, faces):
    first, last = faces[-2:]
    first[n, v, x] = field[0]
    last[n, v, x] = field[-1]
    if count == 2:
        own = lax.axis_index("gx")
        if x == extent_x - 1:

            @pl.when(own == 0)
            def _():
                faces[0][n, v] = field

        if x == 0:

            @pl.when(own == 1)
            def _():
                faces[0][n, v] = field
    else:
        if x == 0:
            faces[0][n, v] = field
        if x == extent_x - 1:
            faces[1][n, v] = field


def faces_body(count, u, *faces):
    local, size, extent_x = u.shape[:3]
    for n in range(local):
        for v in range(size):
            for x in range(extent_x):
                store_faces(u[n, v, x], n, v, x, extent_x, count, faces)


def near_body(ranks, final, omega, coup, u, *refs):
    near, refs = (refs[0], refs[1:]) if ranks > 1 else (None, refs)
    source, refs = refs[0], refs[1:]
    if final:
        jac, out, product = refs
    else:
        (out,) = refs
    local, size, extent_x, extent_y, extent_z = u.shape
    row_at = lax.broadcasted_iota(jnp.int32, (extent_y, extent_z), 0)
    lane_at = lax.broadcasted_iota(jnp.int32, (extent_y, extent_z), 1)
    table = [weights(ranks, local, 0, omega[0])]
    fields = [u]
    if ranks > 1:
        table.append(weights(ranks, local, 1, omega[0]))
        fields.append(near)
    group = math.gcd(GROUP, extent_x)

    def moved(cells, at, edge, shift, axis):
        return [jnp.where(at == edge, 0.0, pltpu.roll(c, shift, axis)) for c in cells]

    for n in range(local):
        for start in range(0, extent_x, group):
            rows = range(start, start + group)
            acc = [[source[n, v, x] for x in rows] for v in range(size)]
            for w in range(size):
                cells = [u[n, w, x] for x in rows]
                below = [u[n, w, start - 1] if start else None] + cells[:-1]
                above = cells[1:] + [u[n, w, start + group] if start + group < extent_x else None]
                around = [
                    below,
                    above,
                    moved(cells, row_at, 0, 1, 0),
                    moved(cells, row_at, extent_y - 1, extent_y - 1, 0),
                    moved(cells, lane_at, 0, 1, 1),
                    moved(cells, lane_at, extent_z - 1, extent_z - 1, 1),
                ]
                for d in range(6):
                    for v in range(size):
                        factor = coup[d, v, w]
                        for k in range(group):
                            if around[d][k] is not None:
                                acc[v][k] = acc[v][k] - factor * around[d][k]
            for field, part in zip(fields, table):
                for j in range(local):
                    factor = part[n][j]
                    if factor is None:
                        continue
                    for v in range(size):
                        for k, x in enumerate(rows):
                            acc[v][k] = acc[v][k] - factor * field[j, v, x]
            for v in range(size):
                for k, x in enumerate(rows):
                    out[n, v, x] = acc[v][k]
            if final:
                for x in rows:
                    for v in range(size):
                        total = jac[n, v, 0, x] * u[n, 0, x]
                        for w in range(1, size):
                            total = total + jac[n, v, w, x] * u[n, w, x]
                        product[n, v, x] = total


def far_body(count, ranks, first, length, final, omega, coup, part, lu, *refs):
    far, refs = refs[: max(ranks - 2, 0)], refs[max(ranks - 2, 0) :]
    gx, refs = (refs[:1], refs[1:]) if count == 2 else (refs[:2], refs[2:])
    low_y, high_y, refs = refs[0], refs[1], refs[2:]
    local, size, extent_x, extent_y, extent_z = part.shape
    done = first + length == extent_x
    product = before = whole = resid = None
    if final:
        product, refs = refs[0], refs[1:]
        if first:
            kept, refs = refs[:2], refs[2:]
        out, resid = refs
    else:
        if first:
            before, refs = refs[0], refs[1:]
        out, refs = refs[0], refs[1:]
        if done:
            whole, faces = refs[0], refs[1:]
    at = first if final and done else 0
    own = lax.axis_index("gx")
    row_at = lax.broadcasted_iota(jnp.int32, (extent_y, extent_z), 0)
    table = [weights(ranks, local, slot, omega[0]) for slot in range(2, ranks)]
    group = math.gcd(GROUP, length)

    def beyond(n, w, side):
        if count == 2:
            return jnp.where(own == 1 - side, gx[0][n, w], 0.0)
        return gx[side][n, w]

    for n in range(local):
        for start in range(first, first + length, group):
            rows = range(start, start + group)
            right = [[part[n, v, x] for x in rows] for v in range(size)]
            for field, entry in zip(far, table):
                for j in range(local):
                    for v in range(size):
                        for k, x in enumerate(rows):
                            right[v][k] = right[v][k] - entry[n][j] * field[j, v, x - first]
            low = [low_y[n, w, start : start + group] for w in range(size)]
            high = [high_y[n, w, start : start + group] for w in range(size)]
            for v in range(size):
                lows = coup[2, v, 0] * low[0]
                highs = coup[3, v, 0] * high[0]
                for w in range(1, size):
                    lows = lows + coup[2, v, w] * low[w]
                    highs = highs + coup[3, v, w] * high[w]
                for k in range(group):
                    edge = jnp.where(row_at == 0, lows[k : k + 1], 0.0)
                    edge = edge + jnp.where(row_at == extent_y - 1, highs[k : k + 1], 0.0)
                    right[v][k] = right[v][k] - edge
            for side, x in enumerate((0, extent_x - 1)):
                if x in rows:
                    for w in range(size):
                        cells = beyond(n, w, side)
                        for v in range(size):
                            right[v][x - start] = right[v][x - start] - coup[side, v, w] * cells
            for k, x in enumerate(rows):
                vector = [right[v][k] for v in range(size)]
                if final:
                    for v in range(size):
                        resid[n, v, x - first + at] = vector[v] - product[n, v, x]
                for p in range(size):
                    for t in range(p + 1, size):
                        vector[t] = vector[t] - lu[n, t, p, x] * vector[p]
                for p in reversed(range(size)):
                    for c in range(p + 1, size):
                        vector[p] = vector[p] - lu[n, p, c, x] * vector[c]
                    vector[p] = vector[p] * lu[n, p, p, x]
                for v in range(size):
                    out[n, v, x - first + at] = vector[v]
                    if whole is not None:
                        whole[n, v, x] = vector[v]
                        store_faces(vector[v], n, v, x, extent_x, count, faces)
    if final and first:
        for old, new in zip(kept, (out, resid)):
            new[:, :, :first] = old[...]
    if before is not None:
        for n in range(local):
            for v in range(size):
                for x in range(first):
                    field = before[n, v, x]
                    whole[n, v, x] = field
                    store_faces(field, n, v, x, extent_x, count, faces)


def call(body, smem, outs, *args):
    return pallas(body, smem, outs, args)


def pallas(body, smem, outs, args):
    return pl.pallas_call(
        body,
        out_shape=outs,
        in_specs=[SMEM] * smem + [VMEM] * (len(args) - smem),
        out_specs=[VMEM] * len(outs),
        compiler_params=pltpu.CompilerParams(vmem_limit_bytes=LIMIT),
    )(*args)


def shards(state, source, jacobian, couplings, omega):
    ranks = lax.axis_size("inst")
    count_x = lax.axis_size("gx")
    count_y = lax.axis_size("gy")
    local, size, extent_x, extent_y, extent_z = state.shape
    assert ranks & (ranks - 1) == 0

    def shape(*dims):
        return jax.ShapeDtypeStruct(dims, jnp.float32)

    face_x = shape(local, size, extent_y, extent_z)
    face_y = shape(local, size, extent_x, extent_z)
    face_shapes = [face_x] * (1 if count_x == 2 else 2) + [face_y] * 2
    full = shape(*state.shape)

    def swap(field, bit):
        return lax.ppermute(field, "inst", [(r, r ^ bit) for r in range(ranks)])

    def exchange(faces):
        ring = [(r, (r + 1) % count_y) for r in range(count_y)]
        back = [(b, a) for a, b in ring]
        first, last = faces[-2:]
        low_y = lax.ppermute(last, "gy", ring)
        high_y = lax.ppermute(first, "gy", back)
        line = [(r, r + 1) for r in range(count_x - 1)]
        if count_x == 2:
            gx = [lax.ppermute(faces[0], "gx", [(0, 1), (1, 0)])]
        else:
            gx = [
                lax.ppermute(faces[1], "gx", line),
                lax.ppermute(faces[0], "gx", [(b, a) for a, b in line]),
            ]
        return gx + [low_y, high_y]

    chunks = 2 if extent_x % 2 == 0 else 1
    length = extent_x // chunks
    firsts = [c * length for c in range(chunks)]
    piece = shape(local, size, length, extent_y, extent_z)
    high_bits = []
    bit = ranks // 2
    while bit > 1:
        high_bits.append(bit)
        bit //= 2

    def spread(field):
        slots = {0: field}
        for bit in high_bits:
            slots.update({slot | bit: swap(value, bit) for slot, value in slots.items()})
        return [slots[slot] for slot in range(2, ranks, 2)]

    current = state
    pieces = [state[:, :, f : f + length] for f in firsts]
    far = [spread(field) for field in pieces]
    faces = call(functools.partial(faces_body, count_x), 0, face_shapes, state)
    (lu,) = call(lu_body, 0, [shape(*jacobian.shape)], jacobian)
    for repeat in range(ITERS):
        final = repeat == ITERS - 1
        around = exchange(faces)
        near = [swap(current, 1)] if ranks > 1 else []
        parts = call(
            functools.partial(near_body, ranks, final),
            2,
            [full] * (2 if final else 1),
            omega,
            couplings,
            current,
            *near,
            source,
            *([jacobian] if final else []),
        )
        pieces, ahead, results = [], [], []
        for c, f in enumerate(firsts):
            tied = pieces[-1:] if not final else results
            lu, parts, tied, evens = lax.optimization_barrier((lu, parts, tied, far[c]))
            if c and not final:
                pieces[-1] = tied[0]
            elif c:
                results = tied
            others = []
            for field in evens:
                others += [field, swap(field, 1)]
            args = [omega, couplings, parts[0], lu, *others, *around]
            if final:
                args += [parts[1], *results]
                outs = [full if c == chunks - 1 else piece] * 2
            else:
                args += pieces
                outs = [piece] + ([full] + face_shapes if c == chunks - 1 else [])
            results = call(
                functools.partial(far_body, count_x, ranks, f, length, final), 2, outs, *args
            )
            if not final:
                pieces.append(results[0])
                ahead.append(spread(results[0]))
        if not final:
            far = ahead
            current, faces = results[1], results[2:]
    return (results[0], results[1])


def solution(mesh):
    return jax.shard_map(
        shards,
        mesh=mesh,
        in_specs=(
            P("inst", None, "gx", "gy", None),
            P("inst", None, "gx", "gy", None),
            P("inst", None, None, "gx", "gy", None),
            P(),
            P(),
        ),
        out_specs=(P("inst", None, "gx", "gy", None), P("inst", None, "gx", "gy", None)),
        check_vma=False,
    )
```

```python
import functools
import math

import jax
import jax.numpy as jnp
import numpy as np
from jax import lax
from jax.experimental import pallas as pl
from jax.experimental.pallas import tpu as pltpu
from jax.sharding import PartitionSpec as P


ITERS = 3
GROUP = 4
LIMIT = 16 * 2**20

VMEM = pl.BlockSpec(memory_space=pltpu.VMEM)
SMEM = pl.BlockSpec(memory_space=pltpu.SMEM)


def table_of(total):
    table = np.zeros((total, total))
    for n in range(total):
        for m in range(total):
            if n != m:
                angle = math.pi * (n - m) / total
                table[n, m] = 0.5 * (-1.0) ** (n - m) * math.cos(angle) / math.sin(angle)
    return table.astype(np.float32)


def weights(ranks, local, slot, omega):
    table = table_of(ranks * local)
    rank = lax.axis_index("inst")
    result = []
    for i in range(local):
        row = []
        for j in range(local):
            if slot == 0 and i == j:
                row.append(None)
                continue
            value = jnp.float32(table[i, slot * local + j])
            for r in range(1, ranks):
                entry = jnp.float32(table[r * local + i, (r ^ slot) * local + j])
                value = jnp.where(rank == r, entry, value)
            row.append(omega * value)
        result.append(row)
    return result


def lu_body(jac, lu):
    local, size, _, extent_x = jac.shape[:4]
    for n in range(local):
        for x in range(extent_x):
            m = [[jac[n, i, j, x] for j in range(size)] for i in range(size)]
            for p in range(size):
                m[p][p] = 1.0 / m[p][p]
                for t in range(p + 1, size):
                    m[t][p] = m[t][p] * m[p][p]
                    for c in range(p + 1, size):
                        m[t][c] = m[t][c] - m[t][p] * m[p][c]
            for i in range(size):
                for j in range(size):
                    lu[n, i, j, x] = m[i][j]


def store_faces(field, n, v, x, extent_x, count, faces):
    first, last = faces[-2:]
    first[n, v, x] = field[0]
    last[n, v, x] = field[-1]
    if count == 2:
        own = lax.axis_index("gx")
        if x == extent_x - 1:

            @pl.when(own == 0)
            def _():
                faces[0][n, v] = field

        if x == 0:

            @pl.when(own == 1)
            def _():
                faces[0][n, v] = field
    else:
        if x == 0:
            faces[0][n, v] = field
        if x == extent_x - 1:
            faces[1][n, v] = field


def faces_body(count, u, *faces):
    local, size, extent_x = u.shape[:3]
    for n in range(local):
        for v in range(size):
            for x in range(extent_x):
                store_faces(u[n, v, x], n, v, x, extent_x, count, faces)


def near_body(count, ranks, final, omega, coup, u, *refs):
    near, refs = (refs[0], refs[1:]) if ranks > 1 else (None, refs)
    if count == 2:
        gx, refs = refs[:1], refs[1:]
    else:
        gx, refs = refs[:2], refs[2:]
    low_y, high_y, source, refs = refs[0], refs[1], refs[2], refs[3:]
    if final:
        jac, out, product = refs
    else:
        (out,) = refs
    local, size, extent_x, extent_y, extent_z = u.shape
    own = lax.axis_index("gx")
    row_at = lax.broadcasted_iota(jnp.int32, (extent_y, extent_z), 0)
    lane_at = lax.broadcasted_iota(jnp.int32, (extent_y, extent_z), 1)
    table = [weights(ranks, local, 0, omega[0])]
    fields = [u]
    if ranks > 1:
        table.append(weights(ranks, local, 1, omega[0]))
        fields.append(near)
    group = math.gcd(GROUP, extent_x)

    def beyond(n, w, side):
        if count == 2:
            return jnp.where(own == 1 - side, gx[0][n, w], 0.0)
        return gx[side][n, w]

    for n in range(local):
        for start in range(0, extent_x, group):
            rows = range(start, start + group)
            acc = [[source[n, v, x] for x in rows] for v in range(size)]
            for w in range(size):
                cells = [u[n, w, x] for x in rows]
                below = [u[n, w, start - 1] if start else beyond(n, w, 0)] + cells[:-1]
                above = cells[1:] + [
                    u[n, w, start + group] if start + group < extent_x else beyond(n, w, 1)
                ]
                around = [
                    below,
                    above,
                    [
                        jnp.where(row_at == 0, low_y[n, w, x][None], pltpu.roll(c, 1, 0))
                        for x, c in zip(rows, cells)
                    ],
                    [
                        jnp.where(
                            row_at == extent_y - 1,
                            high_y[n, w, x][None],
                            pltpu.roll(c, extent_y - 1, 0),
                        )
                        for x, c in zip(rows, cells)
                    ],
                    [jnp.where(lane_at == 0, 0.0, pltpu.roll(c, 1, 1)) for c in cells],
                    [
                        jnp.where(lane_at == extent_z - 1, 0.0, pltpu.roll(c, extent_z - 1, 1))
                        for c in cells
                    ],
                ]
                for d in range(6):
                    for v in range(size):
                        factor = coup[v, d, w]
                        for k in range(group):
                            acc[v][k] = acc[v][k] - factor * around[d][k]
            for field, part in zip(fields, table):
                for j in range(local):
                    factor = part[n][j]
                    if factor is None:
                        continue
                    for v in range(size):
                        for k, x in enumerate(rows):
                            acc[v][k] = acc[v][k] - factor * field[j, v, x]
            for v in range(size):
                for k, x in enumerate(rows):
                    out[n, v, x] = acc[v][k]
            if final:
                for x in rows:
                    for v in range(size):
                        total = jac[n, v, 0, x] * u[n, 0, x]
                        for w in range(1, size):
                            total = total + jac[n, v, w, x] * u[n, w, x]
                        product[n, v, x] = total


def far_body(count, ranks, final, omega, part, lu, *refs):
    far, refs = refs[: max(ranks - 2, 0)], refs[max(ranks - 2, 0) :]
    if final:
        product, out, resid = refs
    else:
        out, faces = refs[0], refs[1:]
    local, size, extent_x = part.shape[:3]
    table = [weights(ranks, local, slot, omega[0]) for slot in range(2, ranks)]
    group = math.gcd(GROUP, extent_x)
    for n in range(local):
        for start in range(0, extent_x, group):
            rows = range(start, start + group)
            right = [[part[n, v, x] for x in rows] for v in range(size)]
            for field, entry in zip(far, table):
                for j in range(local):
                    for v in range(size):
                        for k, x in enumerate(rows):
                            right[v][k] = right[v][k] - entry[n][j] * field[j, v, x]
            if final:
                for v in range(size):
                    for k, x in enumerate(rows):
                        resid[n, v, x] = right[v][k] - product[n, v, x]
            for k, x in enumerate(rows):
                vector = [right[v][k] for v in range(size)]
                for p in range(size):
                    for t in range(p + 1, size):
                        vector[t] = vector[t] - lu[n, t, p, x] * vector[p]
                for p in reversed(range(size)):
                    for c in range(p + 1, size):
                        vector[p] = vector[p] - lu[n, p, c, x] * vector[c]
                    vector[p] = vector[p] * lu[n, p, p, x]
                for v in range(size):
                    out[n, v, x] = vector[v]
                    if not final:
                        store_faces(vector[v], n, v, x, extent_x, count, faces)


def call(body, smem, outs, *args):
    return pallas(body, smem, outs, args)


def pallas(body, smem, outs, args):
    return pl.pallas_call(
        body,
        out_shape=outs,
        in_specs=[SMEM] * smem + [VMEM] * (len(args) - smem),
        out_specs=[VMEM] * len(outs),
        compiler_params=pltpu.CompilerParams(vmem_limit_bytes=LIMIT),
    )(*args)


def shards(state, source, jacobian, couplings, omega):
    ranks = lax.axis_size("inst")
    count_x = lax.axis_size("gx")
    count_y = lax.axis_size("gy")
    local, size, extent_x, extent_y, extent_z = state.shape
    assert ranks & (ranks - 1) == 0

    def shape(*dims):
        return jax.ShapeDtypeStruct(dims, jnp.float32)

    face_x = shape(local, size, extent_y, extent_z)
    face_y = shape(local, size, extent_x, extent_z)
    face_shapes = [face_x] * (1 if count_x == 2 else 2) + [face_y] * 2
    full = shape(*state.shape)

    def swap(field, bit):
        return lax.ppermute(field, "inst", [(r, r ^ bit) for r in range(ranks)])

    def exchange(faces):
        ring = [(r, (r + 1) % count_y) for r in range(count_y)]
        back = [(b, a) for a, b in ring]
        first, last = faces[-2:]
        low_y = lax.ppermute(last, "gy", ring)
        high_y = lax.ppermute(first, "gy", back)
        line = [(r, r + 1) for r in range(count_x - 1)]
        if count_x == 2:
            gx = [lax.ppermute(faces[0], "gx", [(0, 1), (1, 0)])]
        else:
            gx = [
                lax.ppermute(faces[1], "gx", line),
                lax.ppermute(faces[0], "gx", [(b, a) for a, b in line]),
            ]
        return gx + [low_y, high_y]

    current = state
    faces = call(functools.partial(faces_body, count_x), 0, face_shapes, state)
    by_row = jnp.transpose(couplings, (1, 0, 2))
    lu = None
    for repeat in range(ITERS):
        final = repeat == ITERS - 1
        slots = {0: current}
        bit = ranks // 2
        while bit > 1:
            slots.update({slot | bit: swap(field, bit) for slot, field in slots.items()})
            bit //= 2
        if ranks > 1:
            slots[1] = swap(current, 1)
        around = exchange(faces)
        near = [slots[1]] if ranks > 1 else []
        parts = call(
            functools.partial(near_body, count_x, ranks, final),
            2,
            [full] * (2 if final else 1),
            omega,
            by_row,
            current,
            *near,
            *around,
            source,
            *([jacobian] if final else []),
        )
        if lu is None:
            blocks, parts = lax.optimization_barrier((jacobian, parts))
            (lu,) = call(lu_body, 0, [shape(*jacobian.shape)], blocks)
        others = [slots[slot] for slot in range(2, ranks, 2)]
        lu, parts, others = lax.optimization_barrier((lu, parts, others))
        for slot, field in zip(range(2, ranks, 2), others):
            slots[slot] = field
            slots[slot | 1] = swap(field, 1)
        results = call(
            functools.partial(far_body, count_x, ranks, final),
            1,
            [full, full] if final else [full] + face_shapes,
            omega,
            parts[0],
            lu,
            *[slots[slot] for slot in range(2, ranks)],
            *parts[1:],
        )
        current, faces = results[0], results[1:]
    return (current, faces[0])


def solution(mesh):
    return jax.shard_map(
        shards,
        mesh=mesh,
        in_specs=(
            P("inst", None, "gx", "gy", None),
            P("inst", None, "gx", "gy", None),
            P("inst", None, None, "gx", "gy", None),
            P(),
            P(),
        ),
        out_specs=(P("inst", None, "gx", "gy", None), P("inst", None, "gx", "gy", None)),
        check_vma=False,
    )
```
